32 devices in a mesh: gene: 4 (over y, x), prot: 8 (over z, core).
Axes of the slice: x: 2, y: 2, z: 4, core: 2. Of those that a mesh axis runs over, the one named last changes fastest.
Arguments:
- density: float32 [256, 48, 16, 128], P('gene', 'prot'), may hold values from 0 to 2
- levels: float32 [8], replicated, may hold values from 0.1 to 0.9
- rate_index: int32 [256, 3], P('gene'), may hold values from 0 to 7
- on_rate: float32 [8], replicated, may hold values from 0.2 to 3
- off_rate: float32 [8], replicated, may hold values from 0.2 to 3
- gene_order: int32 [4], replicated, may hold values from 0 to 3, each once
Outputs:
- evolved: float32 [256, 48, 16, 128], P('gene', 'prot')
The draws below stay inside these ranges and needn't reach their ends.
Inputs may be any that keep to these rules, and one draw needn't show every extreme that they name: `gene_order`: a permutation of 0 to 3.
All inputs are finite; a program needn't handle non-finite values.
Results may differ from the reference program's by a relative error of at most 0.00002.
Values sent between devices are 32-bit elements; how exact they have to be, the bound alone decides.
A program may use at most 128 MiB of HBM per device.

```python
import math
import jax
import jax.numpy as jnp
from jax import lax

STATE_BITS = 8
LEVELS = 8
BLOCKS = 4
SUBSTEPS = 6
NY = 16
NZ = 128
STATES = 256
NX = 48


def touch_ends(values, stream_key, least, top_value):
    spot = [jax.random.randint(jax.random.fold_in(stream_key, axis), (), 0, length) for axis, length in enumerate(values.shape)]
    widest = values.shape.index(max(values.shape))
    neighbour = spot[:widest] + [(spot[widest] + 1) % values.shape[widest]] + spot[widest + 1:]
    return values.at[tuple(spot)].set(least).at[tuple(neighbour)].set(top_value)


def shard_levels(stream_key, shape, split, least, top_value):
    loudness, own = 1.0, jax.random.fold_in(stream_key, 6)
    for axis_at, parts in split:
        heights = jnp.exp(jax.random.uniform(jax.random.fold_in(own, axis_at), (parts,), jnp.float32, least / len(split), top_value / len(split)))
        loudness = loudness * jnp.repeat(heights, shape[axis_at] // parts).reshape([-1 if axis == axis_at else 1 for axis in range(len(shape))])
    return loudness


def setup_inputs(seed: int = 0) -> dict:
    splits = jax.random.split(jax.random.key(seed), 7)
    return {
        "density": jnp.clip(2.0 * jax.random.uniform(splits[0], (STATES, NX, NY, NZ), jnp.float32) ** shard_levels(splits[0], (STATES, NX, NY, NZ), ((0, 4), (1, 8)), -0.2, 0.2), 0.0, 2.0),
        "levels": jnp.clip(jax.random.uniform(splits[1], (LEVELS,), jnp.float32, 0.1, 0.9), 0.1, 0.9),
        "rate_index": touch_ends(jax.random.randint(splits[2], (STATES, 3), 0, LEVELS), jax.random.fold_in(splits[2], 1), 0, LEVELS - 1).astype(jnp.int32),
        "on_rate": jnp.clip(jnp.exp(jax.random.uniform(splits[3], (STATE_BITS,), jnp.float32, math.log(0.2), math.log(3.0))), 0.2, 3.0),
        "off_rate": jnp.clip(jnp.exp(jax.random.uniform(splits[4], (STATE_BITS,), jnp.float32, math.log(0.2), math.log(3.0))), 0.2, 3.0),
        "gene_order": jax.random.permutation(splits[5], BLOCKS).astype(jnp.int32),
    }


DIFF = 1.0
TIME_STEP = 0.15


def along(field, drift, axis):
    pads = [(0, 0)] * 4
    pads[axis] = (1, 1)
    padded = jnp.pad(field, pads)
    dpad = jnp.pad(drift, pads)
    size = field.shape[axis]
    upper = lax.slice_in_dim(padded, 2, size + 2, axis=axis)
    lower = lax.slice_in_dim(padded, 0, size, axis=axis)
    d_up = lax.slice_in_dim(dpad, 2, size + 2, axis=axis)
    d_low = lax.slice_in_dim(dpad, 0, size, axis=axis)
    return DIFF * (upper - 2.0 * field + lower) - 0.5 * (d_up * upper - d_low * lower)


def diffuse_group(pair):
    group_field, group_level = pair
    coord_x = (jnp.arange(NX, dtype=jnp.float32) + 0.5) / NX
    coord_y = (jnp.arange(NY, dtype=jnp.float32) + 0.5) / NY
    coord_z = (jnp.arange(NZ, dtype=jnp.float32) + 0.5) / NZ
    drift_x = (group_level[:, 0, None] - coord_x[None, :])[:, :, None, None]
    drift_y = (group_level[:, 1, None] - coord_y[None, :])[:, None, :, None]
    drift_z = (group_level[:, 2, None] - coord_z[None, :])[:, None, None, :]

    def one_step(step, field):
        change = along(field, drift_x, 1) + along(field, drift_y, 2) + along(field, drift_z, 3)
        return field + TIME_STEP * change

    return lax.fori_loop(0, SUBSTEPS, one_step, group_field)


def reference(density, levels, rate_index, on_rate, off_rate, gene_order):
    states = density.shape[0]
    groups = 16
    level_of = levels[rate_index]
    coord_x = (jnp.arange(NX, dtype=jnp.float32) + 0.5) / NX
    state_ids = jnp.arange(states, dtype=jnp.int32)
    hill = 0.1 + coord_x ** 2 / (0.09 + coord_x ** 2)
    grouped_level = level_of.reshape((groups, states // groups, 3))
    field = density
    for block in range(BLOCKS):
        grouped = field.reshape((groups, states // groups) + field.shape[1:])
        field = lax.map(diffuse_group, (grouped, grouped_level)).reshape(field.shape)
        bit = (STATE_BITS - 1 - gene_order[block]).astype(jnp.int32)
        mate_ids = jnp.bitwise_xor(state_ids, jnp.left_shift(jnp.int32(1), bit))
        mate = field[mate_ids]
        high = (jnp.bitwise_and(jnp.right_shift(state_ids, bit), 1) == 1)[:, None, None, None]
        act = (on_rate[bit] * hill)[None, :, None, None]
        rate = act + off_rate[bit]
        share = act / rate
        decay = jnp.exp(-rate)
        low_part = jnp.where(high, mate, field)
        high_part = jnp.where(high, field, mate)
        total = low_part + high_part
        new_high = share * total + (high_part - share * total) * decay
        field = jnp.where(high, new_high, total - new_high)
    return field
```

```python
from functools import partial

import jax
import jax.numpy as jnp
from jax import lax
from jax.experimental import pallas as pl
from jax.experimental.pallas import tpu as pltpu
from jax.sharding import PartitionSpec as P

STATE_BITS = 8
BLOCKS = 4
SUBSTEPS = 6
DIFF = 1.0
TIME_STEP = 0.15
TOP = 2**BLOCKS
GROUP = 4
CHUNK = 8
MESH = pl.DeviceIdType.MESH


class Plan:
    def __init__(self, genes, prots, count, width, size_y, size_z):
        self.genes, self.prots = genes, prots
        self.units = count * genes // TOP
        self.mids = count // self.units
        self.split = self.units // genes
        self.slabs = prots // self.split
        self.width, self.size_y, self.size_z = width, size_y, size_z
        self.cells = width * self.split
        self.total_x = width * prots
        self.halo = SUBSTEPS
        self.first = self.halo + 2
        self.layers = self.cells + 2 * self.first
        assert self.split * genes == self.units and self.slabs * self.split == prots
        assert self.cells >= self.halo
        gene_bits = genes.bit_length() - 1
        self.masks = [
            1 << (gene_bits - 1 - k) if k < gene_bits else 1 << (BLOCKS - 1 - (k - gene_bits))
            for k in range(BLOCKS)
        ]


def body(
    pn, x_ref, rate_ref, levels_ref, on_ref, off_ref, order_ref, out_ref,
    buf, land, tab_u, tab_d, tab_y, tab_z, tab_s,
    in_send, in_recv, out_send, out_recv, halo_send, halo_recv,
):
    g, p = lax.axis_index("gene"), lax.axis_index("prot")
    ny = pn.size_y
    q, r = p // pn.slabs, p % pn.slabs
    unit = g * pn.split + q
    part, sub = p // pn.split, p % pn.split
    home = jnp.logical_and(part == r, True)
    has_left, has_right = r > 0, r < pn.slabs - 1

    def rows(layer, n):
        return pl.ds(pl.multiple_of(layer * ny, ny), n * ny)

    def unit_of(k):
        return lax.rem(unit + k, pn.units)

    def in_target(u):
        return (u // pn.split, (u % pn.split) * pn.slabs + part)

    def source_of(k):
        return lax.rem(g * pn.split + sub + k, pn.units)

    def out_target(u):
        return (u // pn.split, r * pn.split + u % pn.split)

    barrier = pltpu.get_barrier_semaphore()

    def greet(k, carry):
        pl.semaphore_signal(barrier, inc=1, device_id=in_target(unit_of(k)), device_id_type=MESH)
        return carry

    def greet_back(k, carry):
        tgt = out_target(lax.rem(g * pn.split + sub + k, pn.units))
        pl.semaphore_signal(barrier, inc=1, device_id=tgt, device_id_type=MESH)
        return carry

    me_source = g * pn.split + sub
    lax.fori_loop(1, pn.units, greet, 0)
    for k in range(pn.units):
        tgt = out_target(k)

        @pl.when(jnp.logical_or(tgt[0] != g, tgt[1] != p))
        def _(tgt=tgt):
            pl.semaphore_signal(barrier, inc=1, device_id=tgt, device_id_type=MESH)

    @pl.when(jnp.logical_not(home))
    def _():
        pl.semaphore_signal(barrier, inc=1, device_id=in_target(unit), device_id_type=MESH)

    @pl.when(has_left)
    def _():
        pl.semaphore_signal(barrier, inc=1, device_id=(g, p - 1), device_id_type=MESH)

    @pl.when(has_right)
    def _():
        pl.semaphore_signal(barrier, inc=1, device_id=(g, p + 1), device_id_type=MESH)

    expected = (
        2 * pn.units - jnp.where(home, 2, 0)
        + jnp.where(has_left, 1, 0) + jnp.where(has_right, 1, 0)
    )
    pl.semaphore_wait(barrier, expected)

    for mid in range(pn.mids):
        for k in range(1, pn.units):
            u = unit_of(k)
            pltpu.make_async_remote_copy(
                src_ref=x_ref.at[mid, u],
                dst_ref=buf.at[0, mid * pn.genes + g, rows(pn.first + sub * pn.width, pn.width)],
                send_sem=in_send.at[mid, u],
                recv_sem=in_recv.at[mid, me_source],
                device_id=in_target(u),
                device_id_type=MESH,
            ).start()
        own_dst = buf.at[0, mid * pn.genes + g, rows(pn.first + sub * pn.width, pn.width)]

        @pl.when(home)
        def _(mid=mid, own_dst=own_dst):
            pltpu.make_async_copy(x_ref.at[mid, unit], own_dst, in_recv.at[mid, me_source]).start()

        @pl.when(jnp.logical_not(home))
        def _(mid=mid, own_dst=own_dst):
            pltpu.make_async_remote_copy(
                src_ref=x_ref.at[mid, unit],
                dst_ref=own_dst,
                send_sem=in_send.at[mid, unit],
                recv_sem=in_recv.at[mid, me_source],
                device_id=in_target(unit),
                device_id_type=MESH,
            ).start()

    nz = pn.size_z
    full = (pn.layers * ny, nz)
    start_x = r * pn.cells
    cell = lax.broadcasted_iota(jnp.int32, full, 0) // ny - pn.first + start_x
    inside = jnp.logical_and(cell >= 0, cell < pn.total_x)
    coord = (cell.astype(jnp.float32) + 0.5) / pn.total_x
    step_x = 1.0 / pn.total_x
    half = 0.5 * TIME_STEP
    yi = lax.broadcasted_iota(jnp.int32, (ny, nz), 0)
    zi = lax.broadcasted_iota(jnp.int32, (8, nz), 1)
    y_at = (yi.astype(jnp.float32) + 0.5) / ny
    z_at = (zi.astype(jnp.float32) + 0.5) / nz

    zero_side = jnp.zeros((pn.first * ny, nz), jnp.float32)

    def tables(t, carry):
        mid, gene = t // pn.genes, t % pn.genes
        at = gene * (pn.mids * pn.units) + mid * pn.units + unit
        lev = [levels_ref[rate_ref[at * 3 + k]] for k in range(3)]
        tab_u[t] = jnp.where(inside, TIME_STEP * DIFF - half * (lev[0] - (coord + step_x)), 0.0)
        tab_d[t] = jnp.where(inside, TIME_STEP * DIFF + half * (lev[0] - (coord - step_x)), 0.0)
        tab_y[t, 0] = jnp.where(yi < ny - 1, TIME_STEP * DIFF - half * (lev[1] - (y_at + 1.0 / ny)), 0.0)
        tab_y[t, 1] = jnp.where(yi > 0, TIME_STEP * DIFF + half * (lev[1] - (y_at - 1.0 / ny)), 0.0)
        tab_z[t, 0] = jnp.where(zi < nz - 1, TIME_STEP * DIFF - half * (lev[2] - (z_at + 1.0 / nz)), 0.0)
        tab_z[t, 1] = jnp.where(zi > 0, TIME_STEP * DIFF + half * (lev[2] - (z_at - 1.0 / nz)), 0.0)
        for side in range(2):
            buf[side, t, rows(0, pn.first)] = zero_side
            buf[side, t, rows(pn.first + pn.cells, pn.first)] = zero_side
        return carry

    lax.fori_loop(0, TOP, tables, 0)

    own = (pn.cells * ny, nz)
    own_cell = lax.broadcasted_iota(jnp.int32, own, 0) // ny + start_x
    own_x = (own_cell.astype(jnp.float32) + 0.5) / pn.total_x
    hill = 0.1 + own_x * own_x / (0.09 + own_x * own_x)
    for b in range(BLOCKS):
        bit = STATE_BITS - 1 - order_ref[b]
        act = on_ref[bit] * hill
        rate = act + off_ref[bit]
        share = act / rate
        decay = jnp.exp(-rate)
        gone = 1.0 - decay
        up = share * gone
        down = (1.0 - share) * gone
        tab_s[b, 0, 0] = 1.0 - up
        tab_s[b, 0, 1] = down
        tab_s[b, 1, 0] = 1.0 - down
        tab_s[b, 1, 1] = up

    def wait_in(mid):
        def one(k, carry):
            gs, js = k // pn.split, k % pn.split
            dst = buf.at[0, mid * pn.genes + gs, rows(pn.first + js * pn.width, pn.width)]
            pltpu.make_async_copy(x_ref.at[0, 0], dst, in_recv.at[mid, k]).wait()
            return carry

        lax.fori_loop(0, pn.units, one, 0)

    groups = TOP // GROUP

    def edge_copies(side, gr):
        states = pl.ds(gr * GROUP, GROUP)
        right = pltpu.make_async_remote_copy(
            src_ref=buf.at[side, states, rows(pn.first + pn.cells - pn.halo, pn.halo)],
            dst_ref=land.at[side, 0, states],
            send_sem=halo_send.at[side, 0, gr],
            recv_sem=halo_recv.at[side, 0, gr],
            device_id=(g, p + 1),
            device_id_type=MESH,
        )
        left = pltpu.make_async_remote_copy(
            src_ref=buf.at[side, states, rows(pn.first, pn.halo)],
            dst_ref=land.at[side, 1, states],
            send_sem=halo_send.at[side, 1, gr],
            recv_sem=halo_recv.at[side, 1, gr],
            device_id=(g, p - 1),
            device_id_type=MESH,
        )
        return left, right

    def send_edges(side, gr):
        left, right = edge_copies(side, gr)
        pl.when(has_left)(left.start)
        pl.when(has_right)(right.start)

    def take_edges(side, gr):
        left, right = edge_copies(side, gr)

        @pl.when(has_left)
        def _():
            right.wait_recv()
            left.wait_send()

        @pl.when(has_right)
        def _():
            left.wait_recv()
            right.wait_send()

        def place(i, carry):
            t = gr * GROUP + i

            @pl.when(has_left)
            def _():
                buf[side, t, rows(pn.first - pn.halo, pn.halo)] = land[side, 0, t]

            @pl.when(has_right)
            def _():
                buf[side, t, rows(pn.first + pn.cells, pn.halo)] = land[side, 1, t]

            return carry

        lax.fori_loop(0, GROUP, place, 0)

    def update(src, dst, t, start, n, cy, cz):
        at = start * ny
        size = n * ny

        def read(off):
            return buf[src, t, pl.ds(at + off, size)]

        here = read(0)
        shape3 = (n, ny, nz)
        out = 0.1 * here if DIFF == 1.0 else (1.0 - 6.0 * TIME_STEP * DIFF) * here
        out = out + tab_u[t, pl.ds(at, size)] * read(ny) + tab_d[t, pl.ds(at, size)] * read(-ny)
        along_y = cy[0][None] * read(1).reshape(shape3) + cy[1][None] * read(-1).reshape(shape3)
        z_next = pltpu.roll(here, nz - 1, 1).reshape(n * ny // 8, 8, nz)
        z_last = pltpu.roll(here, 1, 1).reshape(n * ny // 8, 8, nz)
        along_z = cz[0][None] * z_next + cz[1][None] * z_last
        buf[dst, t, pl.ds(at, size)] = out + along_y.reshape(size, nz) + along_z.reshape(size, nz)

    sides = min(pn.slabs - 1, 2)

    def diffuse(side, t):
        cy = (tab_y[t, 0], tab_y[t, 1])
        cz = (tab_z[t, 0], tab_z[t, 1])
        src, dst = side, 1 - side
        for i in range(SUBSTEPS):
            extra = SUBSTEPS - 1 - i
            if sides == 0:
                begin, n = pn.first, pn.cells
            elif sides == 1:
                begin, n = pn.first - jnp.where(has_left, extra, 0), pn.cells + extra
            else:
                begin, n = pn.first - extra, pn.cells + 2 * extra
            pieces = -(-n // CHUNK)
            done = 0
            for c in range(pieces):
                take = (n - done) // (pieces - c)
                update(src, dst, t, begin + done, take, cy, cz)
                done += take
            src, dst = dst, src

    own_rows = rows(pn.first, pn.cells)

    def switch(b, side, t):
        order = order_ref[b]
        mask = jnp.int32(pn.masks[BLOCKS - 1])
        for k in range(BLOCKS - 1):
            mask = jnp.where(order == k, jnp.int32(pn.masks[k]), mask)
        mate = t ^ mask
        high = jnp.where((t & mask) != 0, 1, 0)
        buf[1 - side, t, own_rows] = (
            tab_s[b, high, 0] * buf[side, t, own_rows] + tab_s[b, high, 1] * buf[side, mate, own_rows]
        )

    waited = 0
    for gr in range(groups):
        need = ((gr + 1) * GROUP - 1) // pn.genes + 1
        while waited < need:
            wait_in(waited)
            waited += 1
        send_edges(0, gr)
        if gr:
            take_edges(0, gr - 1)
            lax.fori_loop(0, GROUP, lambda i, c, gr=gr: (diffuse(0, (gr - 1) * GROUP + i), c)[1], 0)
    take_edges(0, groups - 1)
    lax.fori_loop(0, GROUP, lambda i, c: (diffuse(0, (groups - 1) * GROUP + i), c)[1], 0)

    for b in range(BLOCKS):
        side = b % 2
        after = 1 - side
        last = b == BLOCKS - 1

        def flip(gr, carry, b=b, side=side, after=after, last=last):
            lax.fori_loop(0, GROUP, lambda i, c: (switch(b, side, gr * GROUP + i), c)[1], 0)
            if not last:
                send_edges(after, gr)
            return carry

        def spread(gr, carry, after=after):
            take_edges(after, gr)
            lax.fori_loop(0, GROUP, lambda i, c: (diffuse(after, gr * GROUP + i), c)[1], 0)
            return carry

        if last:
            for gr in range(groups):
                flip(gr, 0)
        else:
            lax.fori_loop(0, groups, flip, 0)
            lax.fori_loop(0, groups, spread, 0)

    fin = BLOCKS % 2

    def out_src(mid, u):
        return buf.at[
            fin, mid * pn.genes + u // pn.split, rows(pn.first + (u % pn.split) * pn.width, pn.width)
        ]

    for mid in range(pn.mids):
        for k in range(pn.units):
            u = lax.rem(unit + k, pn.units)
            tgt = out_target(u)
            mine = jnp.logical_and(tgt[0] == g, tgt[1] == p)

            @pl.when(mine)
            def _(mid=mid, u=u):
                pltpu.make_async_copy(out_src(mid, u), out_ref.at[mid, unit], out_recv.at[mid, unit]).start()

            @pl.when(jnp.logical_not(mine))
            def _(mid=mid, u=u, tgt=tgt):
                pltpu.make_async_remote_copy(
                    src_ref=out_src(mid, u),
                    dst_ref=out_ref.at[mid, unit],
                    send_sem=out_send.at[mid, u],
                    recv_sem=out_recv.at[mid, unit],
                    device_id=tgt,
                    device_id_type=MESH,
                ).start()

    def finish(k, carry):
        tgt = out_target(k)
        for mid in range(pn.mids):
            pltpu.make_async_copy(out_src(mid, 0), out_ref.at[mid, k], out_recv.at[mid, k]).wait()

            @pl.when(jnp.logical_or(tgt[0] != g, tgt[1] != p))
            def _(mid=mid):
                pltpu.make_async_copy(out_src(mid, k), out_ref.at[mid, 0], out_send.at[mid, k]).wait()

            @pl.when(jnp.logical_or(k != unit, jnp.logical_not(home)))
            def _(mid=mid):
                pltpu.make_async_copy(x_ref.at[mid, k], out_src(mid, 0), in_send.at[mid, k]).wait()

        return carry

    lax.fori_loop(0, pn.units, finish, 0)


def local(density, levels, rate_index, on_rate, off_rate, gene_order):
    count, width_x, size_y, size_z = density.shape
    pn = Plan(lax.axis_size("gene"), lax.axis_size("prot"), count, width_x, size_y, size_z)
    rates = lax.all_gather(rate_index.reshape(-1), "gene", tiled=True)
    shape = (pn.mids, pn.units, width_x * size_y, size_z)
    smem = pl.BlockSpec(memory_space=pltpu.SMEM)
    hbm = pl.BlockSpec(memory_space=pl.ANY)
    f32 = jnp.float32
    vec = (pn.layers * size_y, size_z)
    out = pl.pallas_call(
        partial(body, pn),
        out_shape=jax.ShapeDtypeStruct(shape, f32),
        in_specs=[hbm] + [smem] * 5,
        out_specs=hbm,
        scratch_shapes=[
            pltpu.VMEM((2, TOP) + vec, f32),
            pltpu.VMEM((2, 2, TOP, pn.halo * size_y, size_z), f32),
            pltpu.VMEM((TOP,) + vec, f32),
            pltpu.VMEM((TOP,) + vec, f32),
            pltpu.VMEM((TOP, 2, size_y, size_z), f32),
            pltpu.VMEM((TOP, 2, 8, size_z), f32),
            pltpu.VMEM((BLOCKS, 2, 2, pn.cells * size_y, size_z), f32),
            pltpu.SemaphoreType.DMA((pn.mids, pn.units)),
            pltpu.SemaphoreType.DMA((pn.mids, pn.units)),
            pltpu.SemaphoreType.DMA((pn.mids, pn.units)),
            pltpu.SemaphoreType.DMA((pn.mids, pn.units)),
            pltpu.SemaphoreType.DMA((2, 2, TOP // GROUP)),
            pltpu.SemaphoreType.DMA((2, 2, TOP // GROUP)),
        ],
        compiler_params=pltpu.CompilerParams(
            collective_id=0, has_side_effects=True, vmem_limit_bytes=60 * 1024 * 1024
        ),
        name="exchange_evolve",
    )(density.reshape(shape), rates, levels, on_rate, off_rate, gene_order)
    return out.reshape(density.shape)


def solution(mesh):
    in_specs = (P("gene", "prot", None, None), P(), P("gene", None), P(), P(), P())
    out_specs = P("gene", "prot", None, None)
    return jax.shard_map(local, mesh=mesh, in_specs=in_specs, out_specs=out_specs, check_vma=False)
```

```python
from functools import partial

import jax
import jax.numpy as jnp
from jax import lax
from jax.experimental import pallas as pl
from jax.experimental.pallas import tpu as pltpu
from jax.sharding import PartitionSpec as P

STATE_BITS = 8
BLOCKS = 4
SUBSTEPS = 6
DIFF = 1.0
TIME_STEP = 0.15
TOP = 2**BLOCKS
GROUP = 4
CHUNK = 8
MESH = pl.DeviceIdType.MESH


class Plan:
    def __init__(self, genes, prots, count, width, size_y, size_z):
        self.genes, self.prots = genes, prots
        self.units = count * genes // TOP
        self.mids = count // self.units
        self.split = self.units // genes
        self.slabs = prots // self.split
        self.width, self.size_y, self.size_z = width, size_y, size_z
        self.cells = width * self.split
        self.total_x = width * prots
        self.halo = SUBSTEPS
        self.first = self.halo + 2
        self.layers = self.cells + 2 * self.first
        assert self.split * genes == self.units and self.slabs * self.split == prots
        assert self.cells >= self.halo
        gene_bits = genes.bit_length() - 1
        self.masks = [
            1 << (gene_bits - 1 - k) if k < gene_bits else 1 << (BLOCKS - 1 - (k - gene_bits))
            for k in range(BLOCKS)
        ]


def body(
    pn, x_ref, rate_ref, levels_ref, on_ref, off_ref, order_ref, out_ref,
    buf, land, tab_u, tab_d, tab_y, tab_z, tab_s, shift, pair,
    in_send, in_recv, out_send, out_recv, halo_send, halo_recv,
):
    g, p = lax.axis_index("gene"), lax.axis_index("prot")
    ny = pn.size_y
    q, r = p // pn.slabs, p % pn.slabs
    unit = g * pn.split + q
    part, sub = p // pn.split, p % pn.split
    home = jnp.logical_and(part == r, True)
    has_left, has_right = r > 0, r < pn.slabs - 1

    def rows(layer, n):
        return pl.ds(pl.multiple_of(layer * ny, ny), n * ny)

    def unit_of(k):
        return lax.rem(unit + k, pn.units)

    def in_target(u):
        return (u // pn.split, (u % pn.split) * pn.slabs + part)

    def source_of(k):
        return lax.rem(g * pn.split + sub + k, pn.units)

    def out_target(u):
        return (u // pn.split, r * pn.split + u % pn.split)

    barrier = pltpu.get_barrier_semaphore()

    def greet(k, carry):
        pl.semaphore_signal(barrier, inc=1, device_id=in_target(unit_of(k)), device_id_type=MESH)
        return carry

    def greet_back(k, carry):
        tgt = out_target(lax.rem(g * pn.split + sub + k, pn.units))
        pl.semaphore_signal(barrier, inc=1, device_id=tgt, device_id_type=MESH)
        return carry

    me_source = g * pn.split + sub
    lax.fori_loop(1, pn.units, greet, 0)
    for k in range(pn.units):
        tgt = out_target(k)

        @pl.when(jnp.logical_or(tgt[0] != g, tgt[1] != p))
        def _(tgt=tgt):
            pl.semaphore_signal(barrier, inc=1, device_id=tgt, device_id_type=MESH)

    @pl.when(jnp.logical_not(home))
    def _():
        pl.semaphore_signal(barrier, inc=1, device_id=in_target(unit), device_id_type=MESH)

    @pl.when(has_left)
    def _():
        pl.semaphore_signal(barrier, inc=1, device_id=(g, p - 1), device_id_type=MESH)

    @pl.when(has_right)
    def _():
        pl.semaphore_signal(barrier, inc=1, device_id=(g, p + 1), device_id_type=MESH)

    expected = (
        2 * pn.units - jnp.where(home, 2, 0)
        + jnp.where(has_left, 1, 0) + jnp.where(has_right, 1, 0)
    )
    pl.semaphore_wait(barrier, expected)

    for mid in range(pn.mids):
        for k in range(1, pn.units):
            u = unit_of(k)
            pltpu.make_async_remote_copy(
                src_ref=x_ref.at[mid, u],
                dst_ref=buf.at[0, mid * pn.genes + g, rows(pn.first + sub * pn.width, pn.width)],
                send_sem=in_send.at[mid, u],
                recv_sem=in_recv.at[mid, me_source],
                device_id=in_target(u),
                device_id_type=MESH,
            ).start()
        own_dst = buf.at[0, mid * pn.genes + g, rows(pn.first + sub * pn.width, pn.width)]

        @pl.when(home)
        def _(mid=mid, own_dst=own_dst):
            pltpu.make_async_copy(x_ref.at[mid, unit], own_dst, in_recv.at[mid, me_source]).start()

        @pl.when(jnp.logical_not(home))
        def _(mid=mid, own_dst=own_dst):
            pltpu.make_async_remote_copy(
                src_ref=x_ref.at[mid, unit],
                dst_ref=own_dst,
                send_sem=in_send.at[mid, unit],
                recv_sem=in_recv.at[mid, me_source],
                device_id=in_target(unit),
                device_id_type=MESH,
            ).start()

    nz = pn.size_z
    full = (pn.layers * ny, nz)
    start_x = r * pn.cells
    cell = lax.broadcasted_iota(jnp.int32, full, 0) // ny - pn.first + start_x
    inside = jnp.logical_and(cell >= 0, cell < pn.total_x)
    coord = (cell.astype(jnp.float32) + 0.5) / pn.total_x
    step_x = 1.0 / pn.total_x
    half = 0.5 * TIME_STEP
    yi = lax.broadcasted_iota(jnp.int32, (ny, nz), 0)
    zi = lax.broadcasted_iota(jnp.int32, (8, nz), 1)
    y_at = (yi.astype(jnp.float32) + 0.5) / ny
    z_at = (zi.astype(jnp.float32) + 0.5) / nz

    zero_side = jnp.zeros((pn.first * ny, nz), jnp.float32)

    from_z = lax.broadcasted_iota(jnp.int32, (2 * nz, 2 * nz), 0) % nz
    to_z = lax.broadcasted_iota(jnp.int32, (2 * nz, 2 * nz), 1)
    wanted = jnp.where(to_z < nz, to_z + 1, to_z - nz - 1)
    shift[...] = jnp.where(from_z == wanted, 1.0, 0.0).astype(shift.dtype)

    def tables(t, carry):
        mid, gene = t // pn.genes, t % pn.genes
        at = gene * (pn.mids * pn.units) + mid * pn.units + unit
        lev = [levels_ref[rate_ref[at * 3 + k]] for k in range(3)]
        tab_u[t] = jnp.where(inside, TIME_STEP * DIFF - half * (lev[0] - (coord + step_x)), 0.0)
        tab_d[t] = jnp.where(inside, TIME_STEP * DIFF + half * (lev[0] - (coord - step_x)), 0.0)
        tab_y[t, 0] = jnp.where(yi < ny - 1, TIME_STEP * DIFF - half * (lev[1] - (y_at + 1.0 / ny)), 0.0)
        tab_y[t, 1] = jnp.where(yi > 0, TIME_STEP * DIFF + half * (lev[1] - (y_at - 1.0 / ny)), 0.0)
        tab_z[t, 0] = jnp.where(zi < nz - 1, TIME_STEP * DIFF - half * (lev[2] - (z_at + 1.0 / nz)), 0.0)
        tab_z[t, 1] = jnp.where(zi > 0, TIME_STEP * DIFF + half * (lev[2] - (z_at - 1.0 / nz)), 0.0)
        for side in range(2):
            buf[side, t, rows(0, pn.first)] = zero_side
            buf[side, t, rows(pn.first + pn.cells, pn.first)] = zero_side
        return carry

    lax.fori_loop(0, TOP, tables, 0)

    own = (pn.cells * ny, nz)
    own_cell = lax.broadcasted_iota(jnp.int32, own, 0) // ny + start_x
    own_x = (own_cell.astype(jnp.float32) + 0.5) / pn.total_x
    hill = 0.1 + own_x * own_x / (0.09 + own_x * own_x)
    for b in range(BLOCKS):
        bit = STATE_BITS - 1 - order_ref[b]
        act = on_ref[bit] * hill
        rate = act + off_ref[bit]
        share = act / rate
        decay = jnp.exp(-rate)
        gone = 1.0 - decay
        up = share * gone
        down = (1.0 - share) * gone
        tab_s[b, 0, 0] = 1.0 - up
        tab_s[b, 0, 1] = down
        tab_s[b, 1, 0] = 1.0 - down
        tab_s[b, 1, 1] = up

    def wait_in(mid):
        def one(k, carry):
            gs, js = k // pn.split, k % pn.split
            dst = buf.at[0, mid * pn.genes + gs, rows(pn.first + js * pn.width, pn.width)]
            pltpu.make_async_copy(x_ref.at[0, 0], dst, in_recv.at[mid, k]).wait()
            return carry

        lax.fori_loop(0, pn.units, one, 0)

    groups = TOP // GROUP

    def edge_copies(side, gr):
        states = pl.ds(gr * GROUP, GROUP)
        right = pltpu.make_async_remote_copy(
            src_ref=buf.at[side, states, rows(pn.first + pn.cells - pn.halo, pn.halo)],
            dst_ref=land.at[side, 0, states],
            send_sem=halo_send.at[side, 0, gr],
            recv_sem=halo_recv.at[side, 0, gr],
            device_id=(g, p + 1),
            device_id_type=MESH,
        )
        left = pltpu.make_async_remote_copy(
            src_ref=buf.at[side, states, rows(pn.first, pn.halo)],
            dst_ref=land.at[side, 1, states],
            send_sem=halo_send.at[side, 1, gr],
            recv_sem=halo_recv.at[side, 1, gr],
            device_id=(g, p - 1),
            device_id_type=MESH,
        )
        return left, right

    def send_edges(side, gr):
        left, right = edge_copies(side, gr)
        pl.when(has_left)(left.start)
        pl.when(has_right)(right.start)

    def take_edges(side, gr):
        left, right = edge_copies(side, gr)

        @pl.when(has_left)
        def _():
            right.wait_recv()
            left.wait_send()

        @pl.when(has_right)
        def _():
            left.wait_recv()
            right.wait_send()

        def place(i, carry):
            t = gr * GROUP + i

            @pl.when(has_left)
            def _():
                buf[side, t, rows(pn.first - pn.halo, pn.halo)] = land[side, 0, t]

            @pl.when(has_right)
            def _():
                buf[side, t, rows(pn.first + pn.cells, pn.halo)] = land[side, 1, t]

            return carry

        lax.fori_loop(0, GROUP, place, 0)

    def update(src, dst, t, start, n, cy, cz, z_row):
        at = start * ny
        size = n * ny

        def read(off):
            return buf[src, t, pl.ds(at + off, size)]

        here = read(0)
        shape3 = (n, ny, nz)
        out = 0.1 * here if DIFF == 1.0 else (1.0 - 6.0 * TIME_STEP * DIFF) * here
        out = out + tab_u[t, pl.ds(at, size)] * read(ny) + tab_d[t, pl.ds(at, size)] * read(-ny)
        along_y = cy[0][None] * read(1).reshape(shape3) + cy[1][None] * read(-1).reshape(shape3)
        z_next = pair[pl.ds(z_row, size), :nz].reshape(n * ny // 8, 8, nz)
        z_last = pair[pl.ds(z_row, size), nz:].reshape(n * ny // 8, 8, nz)
        along_z = cz[0][None] * z_next + cz[1][None] * z_last
        buf[dst, t, pl.ds(at, size)] = out + along_y.reshape(size, nz) + along_z.reshape(size, nz)

    sides = min(pn.slabs - 1, 2)

    def diffuse(side, gr):
        src, dst = side, 1 - side
        for i in range(SUBSTEPS):
            extra = SUBSTEPS - 1 - i
            if sides == 0:
                begin, n = pn.first, pn.cells
            elif sides == 1:
                begin, n = pn.first - jnp.where(has_left, extra, 0), pn.cells + extra
            else:
                begin, n = pn.first - extra, pn.cells + 2 * extra
            size = n * ny
            here = buf[src, pl.ds(gr * GROUP, GROUP), rows(begin, n)].reshape(GROUP * size, nz)
            high = here.astype(jnp.bfloat16)
            low = (here - high.astype(jnp.float32)).astype(jnp.bfloat16)
            pair[pl.ds(0, GROUP * size)] = jnp.dot(
                jnp.concatenate([high, low], axis=1), shift[...], preferred_element_type=jnp.float32
            )

            def one(j, carry, src=src, dst=dst, begin=begin, n=n, size=size):
                t = gr * GROUP + j
                cy = (tab_y[t, 0], tab_y[t, 1])
                cz = (tab_z[t, 0], tab_z[t, 1])
                pieces = -(-n // CHUNK)
                done = 0
                for c in range(pieces):
                    take = (n - done) // (pieces - c)
                    z_row = pl.multiple_of(j * size + done * ny, ny)
                    update(src, dst, t, begin + done, take, cy, cz, z_row)
                    done += take
                return carry

            lax.fori_loop(0, GROUP, one, 0)
            src, dst = dst, src

    own_rows = rows(pn.first, pn.cells)

    def switch(b, side, t):
        order = order_ref[b]
        mask = jnp.int32(pn.masks[BLOCKS - 1])
        for k in range(BLOCKS - 1):
            mask = jnp.where(order == k, jnp.int32(pn.masks[k]), mask)
        mate = t ^ mask
        high = jnp.where((t & mask) != 0, 1, 0)
        buf[1 - side, t, own_rows] = (
            tab_s[b, high, 0] * buf[side, t, own_rows] + tab_s[b, high, 1] * buf[side, mate, own_rows]
        )

    fin = BLOCKS % 2

    def out_src(mid, u):
        return buf.at[
            fin, mid * pn.genes + u // pn.split, rows(pn.first + (u % pn.split) * pn.width, pn.width)
        ]

    def send_out(mid):
        for k in range(pn.units):
            u = lax.rem(unit + k, pn.units)
            tgt = out_target(u)
            mine = jnp.logical_and(tgt[0] == g, tgt[1] == p)

            @pl.when(mine)
            def _(mid=mid, u=u):
                pltpu.make_async_copy(out_src(mid, u), out_ref.at[mid, unit], out_recv.at[mid, unit]).start()

            @pl.when(jnp.logical_not(mine))
            def _(mid=mid, u=u, tgt=tgt):
                pltpu.make_async_remote_copy(
                    src_ref=out_src(mid, u),
                    dst_ref=out_ref.at[mid, unit],
                    send_sem=out_send.at[mid, u],
                    recv_sem=out_recv.at[mid, unit],
                    device_id=tgt,
                    device_id_type=MESH,
                ).start()

    stepwise = pn.genes == GROUP
    if not stepwise:
        for mid in range(pn.mids):
            wait_in(mid)

    def first_block(gr, carry):
        @pl.when(gr < groups)
        def _():
            if stepwise:
                wait_in(gr)
            send_edges(0, gr)

        @pl.when(gr > 0)
        def _():
            take_edges(0, gr - 1)
            diffuse(0, gr - 1)

        return carry

    lax.fori_loop(0, groups + 1, first_block, 0)

    def next_block(b, carry):
        side = lax.rem(b, 2)
        after = 1 - side

        def flip(gr, c):
            lax.fori_loop(0, GROUP, lambda i, k: (switch(b, side, gr * GROUP + i), k)[1], 0)
            send_edges(after, gr)
            return c

        def spread(gr, c):
            take_edges(after, gr)
            diffuse(after, gr)
            return c

        lax.fori_loop(0, groups, flip, 0)
        lax.fori_loop(0, groups, spread, 0)
        return carry

    lax.fori_loop(0, BLOCKS - 1, next_block, 0)

    for gr in range(groups):
        lax.fori_loop(
            0, GROUP,
            lambda i, k, gr=gr: (switch(BLOCKS - 1, (BLOCKS - 1) % 2, gr * GROUP + i), k)[1], 0,
        )
        if stepwise:
            send_out(gr)
    if not stepwise:
        for mid in range(pn.mids):
            send_out(mid)

    def finish(k, carry):
        tgt = out_target(k)
        for mid in range(pn.mids):
            pltpu.make_async_copy(out_src(mid, 0), out_ref.at[mid, k], out_recv.at[mid, k]).wait()

            @pl.when(jnp.logical_or(tgt[0] != g, tgt[1] != p))
            def _(mid=mid):
                pltpu.make_async_copy(out_src(mid, k), out_ref.at[mid, 0], out_send.at[mid, k]).wait()

            @pl.when(jnp.logical_or(k != unit, jnp.logical_not(home)))
            def _(mid=mid):
                pltpu.make_async_copy(x_ref.at[mid, k], out_src(mid, 0), in_send.at[mid, k]).wait()

        return carry

    lax.fori_loop(0, pn.units, finish, 0)


def local(density, levels, rate_index, on_rate, off_rate, gene_order):
    count, width_x, size_y, size_z = density.shape
    pn = Plan(lax.axis_size("gene"), lax.axis_size("prot"), count, width_x, size_y, size_z)
    rates = lax.all_gather(rate_index.reshape(-1), "gene", tiled=True)
    shape = (pn.mids, pn.units, width_x * size_y, size_z)
    smem = pl.BlockSpec(memory_space=pltpu.SMEM)
    hbm = pl.BlockSpec(memory_space=pl.ANY)
    f32 = jnp.float32
    vec = (pn.layers * size_y, size_z)
    out = pl.pallas_call(
        partial(body, pn),
        out_shape=jax.ShapeDtypeStruct(shape, f32),
        in_specs=[hbm] + [smem] * 5,
        out_specs=hbm,
        scratch_shapes=[
            pltpu.VMEM((2, TOP) + vec, f32),
            pltpu.VMEM((2, 2, TOP, pn.halo * size_y, size_z), f32),
            pltpu.VMEM((TOP,) + vec, f32),
            pltpu.VMEM((TOP,) + vec, f32),
            pltpu.VMEM((TOP, 2, size_y, size_z), f32),
            pltpu.VMEM((TOP, 2, 8, size_z), f32),
            pltpu.VMEM((BLOCKS, 2, 2, pn.cells * size_y, size_z), f32),
            pltpu.VMEM((2 * size_z, 2 * size_z), jnp.bfloat16),
            pltpu.VMEM((GROUP * vec[0], 2 * size_z), f32),
            pltpu.SemaphoreType.DMA((pn.mids, pn.units)),
            pltpu.SemaphoreType.DMA((pn.mids, pn.units)),
            pltpu.SemaphoreType.DMA((pn.mids, pn.units)),
            pltpu.SemaphoreType.DMA((pn.mids, pn.units)),
            pltpu.SemaphoreType.DMA((2, 2, TOP // GROUP)),
            pltpu.SemaphoreType.DMA((2, 2, TOP // GROUP)),
        ],
        compiler_params=pltpu.CompilerParams(
            collective_id=0, has_side_effects=True, vmem_limit_bytes=60 * 1024 * 1024
        ),
        name="exchange_evolve",
    )(density.reshape(shape), rates, levels, on_rate, off_rate, gene_order)
    return out.reshape(density.shape)


def solution(mesh):
    in_specs = (P("gene", "prot", None, None), P(), P("gene", None), P(), P(), P())
    out_specs = P("gene", "prot", None, None)
    return jax.shard_map(local, mesh=mesh, in_specs=in_specs, out_specs=out_specs, check_vma=False)
```
